32 devices in a mesh: groups: 2 (over x), seq: 16 (over z, y, core).
Axes of the slice: x: 2, y: 2, z: 4, core: 2. Of those that a mesh axis runs over, the one named last changes fastest.
Arguments:
- queries: bfloat16 [8192, 4096], P(('groups', 'seq')), parts along dimension 0, may hold values from -6 to 6
- keys: bfloat16 [8192, 2048], P(('groups', 'seq')), parts along dimension 0, may hold values from -6 to 6
- values: bfloat16 [8192, 2048], P(('groups', 'seq')), parts along dimension 0, may hold values from -6 to 6
- doc_blocks: int32 [16], P('groups'), parts along dimension 0, may hold values from 1 to 8, 32 in all
Outputs:
- attended: bfloat16 [8192, 4096], P(('groups', 'seq')), parts along dimension 0
The draws below stay inside these ranges and needn't reach their ends.
There are 2 independent parts, one for each index of `groups`. The reference program is written for one: setup_inputs(seed, part) draws one part's arguments, and reference() takes and returns one part's arrays. A program takes and returns all parts, laid end to end along the dimension named above; each array names one. Nothing has to cross between parts.
Inputs may be any that keep to these rules, and one draw needn't show every extreme that they name: `doc_blocks`: the lengths add up to 32; the longest document has exactly 8 units.
All inputs are finite; a program needn't handle non-finite values.
Results may differ from the reference program's by a relative error of at most 0.004.
Values may be sent and summed in bfloat16 or wider, within the bound.
A program may use at most 64 MiB of HBM per device.

```python
import math
import jax
import jax.numpy as jnp
import numpy as np
from jax import lax

HEADS = 32
KV_HEADS = 16
DH = 128
BLK = 128
DOCS = 8
TOKENS = 4096


def draw_keys(key, part):
    own_key = jax.random.fold_in(key, 11)
    background = jnp.clip(jax.random.normal(own_key, (TOKENS, KV_HEADS * DH), jnp.float32), -6.0, 6.0)
    return background.astype(jnp.bfloat16)


def draw_queries(key, part):
    own_key = jax.random.fold_in(key, 17)
    background = jnp.clip(jax.random.normal(own_key, (TOKENS, HEADS * DH), jnp.float32), -6.0, 6.0)
    return background.astype(jnp.bfloat16)


def levels(key, dims, pieces, low, high):
    def one(dim, shards_of):
        draws = jax.random.uniform(jax.random.fold_in(jax.random.fold_in(key, 6), dim), (shards_of,), jnp.float32, low / len(pieces), high / len(pieces))
        return jnp.repeat(jnp.exp(draws), dims[dim] // shards_of).reshape((-1,) + (1,) * (len(dims) - dim - 1))

    loudness = one(*pieces[0])
    for cut in pieces[1:]:
        loudness = loudness * one(*cut)
    return loudness


def length_profile(amount, total, most, slope):
    portions = [(1 << 20) // math.isqrt(rank ** slope) + 1 for rank in range(2, amount + 1)]
    spare, counts = total - most - (amount - 1), [1] * (amount - 1)
    while spare > 0:
        movable = [i for i in range(amount - 1) if counts[i] < most]
        mass, budget = sum([portions[i] for i in movable]), spare
        for i in movable:
            extra = min(most - counts[i], max(1, budget * portions[i] // mass), spare)
            counts[i] = counts[i] + extra
            spare = spare - extra
    return np.array([most] + counts)


def ragged_sizes(stream_key, number_of, total, limit, lean):
    if number_of == 2:
        one = jax.random.randint(stream_key, (), max(1, total - limit), min(limit, total - 1) + 1)
        return jnp.stack([one, total - one])
    tallies = jnp.asarray(length_profile(number_of, total, limit, lean), jnp.int32)
    twos = (number_of - 1) // 2
    source_of, sink = tallies[1:1 + 2 * twos:2], tallies[2:2 + 2 * twos:2]
    margin = jnp.minimum(source_of - 1, limit - sink)
    shifted = jax.random.randint(jax.random.fold_in(stream_key, 1), (twos,), 0, 1 << 20) % (margin + 1)
    tallies = tallies.at[1:1 + 2 * twos:2].set(source_of - shifted).at[2:2 + 2 * twos:2].set(sink + shifted)
    return tallies[jax.random.permutation(jax.random.fold_in(stream_key, 2), number_of)]


def bell_draw(key, dims, width, most, pieces=(), held_as=jnp.bfloat16):
    gain = levels(key, dims, pieces, -0.22, 0.18) if pieces else 1.0
    entries = jax.random.normal(key, dims, jnp.float32) * width * gain
    return jnp.minimum(jnp.maximum(entries, -most), most).astype(held_as)


def setup_inputs(seed: int = 0, part: int = 0) -> dict:
    key_list = jax.random.split(jax.random.key(seed), 5)
    own_keys = jax.random.split(jax.random.fold_in(key_list[4], part), 5)
    queries = draw_queries(jax.random.fold_in(jax.random.fold_in(key_list[4], part), 71), part)
    keys = draw_keys(jax.random.fold_in(jax.random.fold_in(key_list[4], part), 71), part)
    values = bell_draw(own_keys[2], (TOKENS, KV_HEADS * DH), 1.0, 6.0, ((0, 16),))
    doc_blocks = ragged_sizes(own_keys[3], DOCS, TOKENS // BLK, TOKENS // BLK // 4, 2).astype(jnp.int32)
    return dict(queries=queries, keys=keys, values=values, doc_blocks=doc_blocks)


score_scale = 144.0 ** -0.5


def reference(queries, keys, values, doc_blocks):
    lengths = doc_blocks.astype(jnp.int32) * BLK
    doc_ends = jnp.cumsum(lengths).astype(jnp.int32)
    doc_starts = (doc_ends - lengths).astype(jnp.int32)
    positions = jnp.arange(TOKENS, dtype=jnp.int32)
    doc_number = jnp.sum((positions[:, None] >= doc_ends[None, :]).astype(jnp.int32), axis=1).astype(jnp.int32)
    own_start = jnp.sum(jnp.where(doc_number[:, None] == jnp.arange(DOCS, dtype=jnp.int32)[None, :], doc_starts[None, :], 0), axis=1).astype(jnp.int32)
    query_heads = queries.reshape(TOKENS, KV_HEADS, HEADS // KV_HEADS, DH)
    key_heads = keys.reshape(TOKENS, KV_HEADS, DH)
    value_heads = values.reshape(TOKENS, KV_HEADS, DH)
    tile_rows = min(256, TOKENS)
    window_rows = min(TOKENS, TOKENS // 4 + tile_rows)

    def one_tile(block_index):
        first_row = (block_index * tile_rows).astype(jnp.int32)
        query_tile = lax.dynamic_slice_in_dim(query_heads, first_row, tile_rows, 0).astype(jnp.float32)
        key_first = jnp.clip(first_row + tile_rows - window_rows, 0, TOKENS - window_rows).astype(jnp.int32)
        key_tile = lax.dynamic_slice_in_dim(key_heads, key_first, window_rows, 0).astype(jnp.float32)
        value_tile = lax.dynamic_slice_in_dim(value_heads, key_first, window_rows, 0).astype(jnp.float32)
        scores = jnp.einsum("qgsd,kgd->gsqk", query_tile, key_tile) * score_scale
        tile_pos = first_row + jnp.arange(tile_rows, dtype=jnp.int32)
        tile_start = lax.dynamic_slice_in_dim(own_start, first_row, tile_rows, 0)
        key_pos = key_first + jnp.arange(window_rows, dtype=jnp.int32)
        visible = (key_pos[None, :] >= tile_start[:, None]) & (key_pos[None, :] <= tile_pos[:, None])
        row_max = jnp.max(jnp.where(visible, scores, -1e30), axis=-1)
        weights = jnp.where(visible, jnp.exp(scores - row_max[..., None]), 0.0)
        row_total = jnp.sum(weights, axis=-1)
        rounded = lax.optimization_barrier(weights.astype(jnp.bfloat16)).astype(jnp.float32)
        blended = jnp.einsum("gsqk,kgd->gsqd", rounded, value_tile) / row_total[..., None]
        return blended.transpose(2, 0, 1, 3).reshape(tile_rows, HEADS * DH).astype(jnp.bfloat16)

    blocks = lax.map(one_tile, jnp.arange(TOKENS // tile_rows, dtype=jnp.int32))
    return blocks.reshape(TOKENS, HEADS * DH)
```

```python
import functools

import jax
import jax.numpy as jnp
from jax import lax
from jax.experimental import pallas as pl
from jax.experimental.pallas import tpu as pltpu
from jax.sharding import PartitionSpec as P

DH = 128
BLK = 128
CHUNK_HEADS = 1
ROUTED = 1
EXP2_SCALE = 144.0 ** (-0.5) * 1.4426950408889634
HIDDEN = -1e30
ROUTED_STEP = 6
CROSS_AHEAD = 4
UP_AHEAD = 3


def kernel(
    n,
    window,
    docs_ref,
    q_hbm,
    k_hbm,
    v_hbm,
    o_own,
    q_own,
    k_own,
    v_own,
    k_halo,
    v_halo,
    local_sem,
    send_sem,
    recv_sem,
    k_transit,
    v_transit,
    transit_send,
    transit_recv,
    forward_send,
):
    me = lax.axis_index("seq")
    pairs = window // 2
    place = lax.rem(me, window)
    base = me - place
    pair = place // 2
    core = lax.rem(me, 2)
    partner = me + 1 - 2 * core
    above = me + window
    below = me - window
    has_above = above < n
    has_below = below >= 0

    rows, kv_width = k_hbm.shape
    ratio = q_hbm.shape[1] // kv_width
    width = CHUNK_HEADS * DH
    chunks = kv_width // width
    blocks = rows // BLK
    own_hbm = (k_hbm, v_hbm)
    halo = (k_halo, v_halo)
    transit = (k_transit, v_transit)
    first_routed = chunks - ROUTED

    def pair_device(step):
        return base + 2 * lax.rem(pair + step, pairs) + core

    def kv_cols(c):
        return pl.ds(pl.multiple_of(c * width, width), width)

    def remote_one(kind, c, src_slot, dst_slot, device, from_row=0):
        taken = pl.ds(from_row, rows - from_row)
        if src_slot is None:
            src = own_hbm[kind].at[taken, kv_cols(c)]
        else:
            src = halo[kind].at[src_slot, taken, kv_cols(c)]
        return pltpu.make_async_remote_copy(
            src_ref=src,
            dst_ref=halo[kind].at[dst_slot, taken, kv_cols(c)],
            send_sem=send_sem.at[kind, dst_slot, c],
            recv_sem=recv_sem.at[kind, dst_slot, c],
            device_id={"seq": device},
            device_id_type=pl.DeviceIdType.MESH,
        )

    def is_routed(c):
        return (c >= first_routed) & (c < first_routed + ROUTED)

    def turn(spot):
        moved = jnp.where(spot < chunks - 1, spot + 1, first_routed - 1)
        return jnp.where((pair == 0) & (spot >= first_routed - 1), moved, spot)

    def across(kind, c, step):
        spot = c - first_routed
        return pltpu.make_async_remote_copy(
            src_ref=own_hbm[kind].at[:, kv_cols(c)],
            dst_ref=transit[kind].at[step - 1, spot],
            send_sem=transit_send.at[kind, step - 1, spot],
            recv_sem=transit_recv.at[kind, step - 1, spot],
            device_id={"seq": pair_device(step)},
            device_id_type=pl.DeviceIdType.MESH,
        )

    def forward(kind, c, step):
        spot = c - first_routed
        return pltpu.make_async_remote_copy(
            src_ref=transit[kind].at[step - 1, spot],
            dst_ref=halo[kind].at[2 * step, :, kv_cols(c)],
            send_sem=forward_send.at[kind, step - 1, spot],
            recv_sem=recv_sem.at[kind, 2 * step, c],
            device_id={"seq": above},
            device_id_type=pl.DeviceIdType.MESH,
        )

    def remote(c, src_slot, dst_slot, device):
        return [remote_one(kind, c, src_slot, dst_slot, device) for kind in range(2)]

    def upward(kind, c, act):
        @pl.when(place == 0)
        def _():
            act(remote_one(kind, c, None, 0, above, BLK))

        @pl.when(place != 0)
        def _():
            act(remote_one(kind, c, None, 0, above))

    def start(copies):
        for copy in copies:
            copy.start()

    def partner_slot(step):
        return lax.rem(2 * step + 1 - 2 * core + window, window)

    barrier = pltpu.get_barrier_semaphore()

    def greet(device):
        pl.semaphore_signal(
            barrier, inc=1, device_id={"seq": device}, device_id_type=pl.DeviceIdType.MESH
        )

    greet(partner)
    for step in range(1, pairs):
        greet(pair_device(step))

    @pl.when(has_above)
    def _():
        greet(above)

    @pl.when(has_below)
    def _():
        greet(below)

    local = [
        pltpu.make_async_copy(k_hbm, k_own, local_sem.at[0]),
        pltpu.make_async_copy(v_hbm, v_own, local_sem.at[1]),
        pltpu.make_async_copy(q_hbm, q_own, local_sem.at[2]),
    ]
    start(local)
    pl.semaphore_wait(
        barrier, pairs + has_above.astype(jnp.int32) + has_below.astype(jnp.int32)
    )

    def cross_first(spot, carry):
        for step in range(1, pairs):

            @pl.when((pair + step >= pairs) & has_above)
            def _():
                for kind in range(2):
                    across(kind, first_routed + spot, step).start()

        return carry

    lax.fori_loop(0, ROUTED, cross_first, 0)

    def first_sends(c, carry):
        @pl.when(has_above)
        def _():
            for kind in range(2):
                upward(kind, c, lambda copy: copy.start())

        for step in range(1, pairs):

            @pl.when(pair + step < pairs)
            def _():
                start(remote(c, None, 2 * step, pair_device(step)))

        @pl.when(core == 0)
        def _():
            start(remote(c, None, 1, partner))

        return carry

    lax.fori_loop(0, chunks, first_sends, 0)

    @pl.when(jnp.logical_not(has_below))
    def _():
        for r in range(window):

            @pl.when((r == 0) | (r > place))
            def _():
                def clear(i, carry):
                    taken = pl.ds(pl.multiple_of(i * 16, 16), 16)
                    for ref in halo:
                        ref[r, taken, :] = jnp.zeros((16, kv_width), ref.dtype)
                    return carry

                lax.fori_loop(0, rows // 16, clear, 0)

    hide_rows = []
    for a in range(blocks):
        number = me * blocks + a
        end = jnp.int32(0)
        first = jnp.int32(0)
        for d in range(docs_ref.shape[0]):
            end = end + docs_ref[d]
            first = jnp.where(end <= number, end, first)
        held = [(me - window) * blocks + b for b in range(a + 1, blocks)]
        for r in range(1, window):
            held += [(me - r) * blocks + b for b in range(blocks)]
        held += [me * blocks + b for b in range(a + 1)]
        hide_rows.append(
            jnp.concatenate(
                [
                    jnp.full((1, BLK), jnp.where(b >= first, 0.0, HIDDEN), jnp.float32)
                    for b in held
                ],
                axis=1,
            )
        )

    for copy in local:
        copy.wait()

    def attend(c):
        q_index = lax.broadcasted_iota(jnp.int32, (BLK, BLK), 0)
        k_index = lax.broadcasted_iota(jnp.int32, (BLK, BLK), 1)
        causal = jnp.where(k_index <= q_index, 0.0, HIDDEN).astype(jnp.float32)
        causal = jnp.concatenate([causal] * ratio, axis=0)
        for h in range(CHUNK_HEADS):
            cols = pl.ds(pl.multiple_of(c * width + h * DH, DH), DH)
            for a in range(blocks):
                own_rows = (a + 1) * BLK

                def gathered(halo_ref, own_ref):
                    parts = []
                    if own_rows < rows:
                        parts.append(halo_ref[0, own_rows:, cols])
                    for r in range(1, window):
                        parts.append(halo_ref[r, :, cols])
                    parts.append(own_ref[:own_rows, cols])
                    return jnp.concatenate(parts, axis=0)

                head_cols = [
                    pl.ds(pl.multiple_of((c * width + h * DH) * ratio + g * DH, DH), DH)
                    for g in range(ratio)
                ]
                tile_rows = slice(a * BLK, (a + 1) * BLK)
                q_tile = jnp.concatenate([q_own[tile_rows, hc] for hc in head_cols], axis=0)
                scores = lax.dot_general(
                    q_tile,
                    gathered(k_halo, k_own),
                    (((1,), (1,)), ((), ())),
                    preferred_element_type=jnp.float32,
                )
                scores = scores + hide_rows[a]
                scores = jnp.concatenate([scores[:, :-BLK], scores[:, -BLK:] + causal], axis=1)
                top = jnp.max(scores, axis=1, keepdims=True)
                weights = jnp.exp2((scores - top) * EXP2_SCALE)
                total = jnp.sum(weights, axis=1, keepdims=True)
                blended = jnp.dot(
                    weights.astype(jnp.bfloat16),
                    gathered(v_halo, v_own),
                    preferred_element_type=jnp.float32,
                )
                blended = (blended / total).astype(o_own.dtype)
                for g in range(ratio):
                    o_own[tile_rows, head_cols[g]] = blended[g * BLK : (g + 1) * BLK]

    def arrived(c, slot):
        for copy in remote(c, None, slot, partner):
            copy.wait_recv()

    def step_of(t, carry):
        @pl.when((t < chunks) & has_below)
        def _():
            c = t
            for kind in range(2):
                upward(kind, c, lambda copy: copy.wait_recv())

                @pl.when(core == 1)
                def _():
                    remote_one(kind, c, 0, window - 1, partner).start()

                for step in range(1, pairs):

                    @pl.when((pair + step >= pairs) & jnp.logical_not(is_routed(c)))
                    def _():
                        remote_one(kind, c, 0, 2 * step, pair_device(step)).start()

        @pl.when((t < ROUTED) & has_above)
        def _():
            for step in range(1, pairs):

                @pl.when(step > pair)
                def _():
                    for kind in range(2):
                        across(kind, t + first_routed, step).wait_recv()
                        forward(kind, t + first_routed, step).start()

        @pl.when((t >= 1) & (t < chunks + 1))
        def _():
            c = turn(t - 1)
            for step in range(1, pairs):

                @pl.when((pair >= step) | has_below)
                def _():
                    for kind in range(2):
                        remote_one(kind, c, None, 2 * step, partner).wait_recv()
                        remote_one(kind, c, 2 * step, partner_slot(step), partner).start()

        @pl.when((t >= 2) & (t < chunks + 2))
        def _():
            c = turn(t - 2)
            for r in range(1, window, 2):

                @pl.when((place >= r) | has_below)
                def _():
                    arrived(c, r)

            attend(c)

        return carry

    lax.fori_loop(0, chunks + 2, step_of, 0)

    def finish(c, carry):
        def sent(slot):
            for copy in remote(c, None, slot, partner):
                copy.wait_send()

        @pl.when(has_above)
        def _():
            for kind in range(2):
                upward(kind, c, lambda copy: copy.wait_send())

        @pl.when((core == 0) | has_below)
        def _():
            sent(partner_slot(0))

        for step in range(1, pairs):

            @pl.when((pair + step < pairs) | (has_below & jnp.logical_not(is_routed(c))))
            def _():
                sent(2 * step)

            @pl.when((pair + step >= pairs) & has_above & is_routed(c))
            def _():
                for kind in range(2):
                    across(kind, c, step).wait_send()

            @pl.when((step > pair) & has_above & is_routed(c))
            def _():
                for kind in range(2):
                    forward(kind, c, step).wait_send()

            @pl.when((pair >= step) | has_below)
            def _():
                sent(partner_slot(step))

        return carry

    lax.fori_loop(0, chunks, finish, 0)


def on_device(n, queries, keys, values, doc_blocks):
    window = n // 4
    rows, kv_width = keys.shape
    chunks = kv_width // (CHUNK_HEADS * DH)
    return pl.pallas_call(
        functools.partial(kernel, n, window),
        out_shape=pltpu.VMEM(queries.shape, queries.dtype),
        in_specs=[pl.BlockSpec(memory_space=pltpu.SMEM)]
        + [pl.BlockSpec(memory_space=pl.ANY)] * 3,
        out_specs=pl.BlockSpec(memory_space=pltpu.VMEM),
        scratch_shapes=[
            pltpu.VMEM(queries.shape, queries.dtype),
            pltpu.VMEM(keys.shape, keys.dtype),
            pltpu.VMEM(values.shape, values.dtype),
            pltpu.VMEM((window, rows, kv_width), keys.dtype),
            pltpu.VMEM((window, rows, kv_width), values.dtype),
            pltpu.SemaphoreType.DMA((3,)),
            pltpu.SemaphoreType.DMA((2, window, chunks)),
            pltpu.SemaphoreType.DMA((2, window, chunks)),
            pltpu.VMEM((window // 2 - 1, ROUTED, rows, CHUNK_HEADS * DH), keys.dtype),
            pltpu.VMEM((window // 2 - 1, ROUTED, rows, CHUNK_HEADS * DH), values.dtype),
            pltpu.SemaphoreType.DMA((2, window // 2 - 1, ROUTED)),
            pltpu.SemaphoreType.DMA((2, window // 2 - 1, ROUTED)),
            pltpu.SemaphoreType.DMA((2, window // 2 - 1, ROUTED)),
        ],
        compiler_params=pltpu.CompilerParams(
            collective_id=0, has_side_effects=True, vmem_limit_bytes=60 * 1024 * 1024
        ),
    )(doc_blocks, queries, keys, values)


def paired_kernel(
    n,
    docs_ref,
    q_hbm,
    k_hbm,
    v_hbm,
    o_own,
    q_own,
    k_own,
    v_own,
    k_halo,
    v_halo,
    k_transit,
    v_transit,
    local_sem,
    send_sem,
    recv_sem,
    transit_send,
    transit_recv,
    first_send,
    first_recv,
):
    me = lax.axis_index("seq")
    place = lax.rem(me, 4)
    row = me // 4
    last_row = n // 4 - 1
    far = place // 2
    core = lax.rem(me, 2)
    partner = me + 1 - 2 * core
    across = me + 2 - 4 * far
    above = me + 4
    below = me - 4
    has_above = above < n
    has_below = below >= 0

    rows, kv_width = k_hbm.shape
    ratio = q_hbm.shape[1] // kv_width
    chunks = kv_width // DH
    blocks = rows // BLK
    own_hbm = (k_hbm, v_hbm)
    halo = (k_halo, v_halo)
    transit = (k_transit, v_transit)
    early = jnp.where(core == 0, 3, 1)
    late = 4 - early
    has_far = (far == 1) | has_below

    def first_routed(of_row):
        return chunks - jnp.minimum(chunks, ROUTED_STEP * (last_row - of_row))

    own_first = first_routed(row)
    below_first = first_routed(row - 1)
    tops = slice(0, BLK)
    lows = slice(BLK, rows)
    whole = slice(0, rows)

    def kv_cols(c):
        return pl.ds(pl.multiple_of(c * DH, DH), DH)

    def copy_of(kind, src, dst, c, taken, device):
        if src is None:
            src_ref = own_hbm[kind].at[taken, kv_cols(c)]
        else:
            src_ref = halo[kind].at[src, taken, kv_cols(c)]
        return pltpu.make_async_remote_copy(
            src_ref=src_ref,
            dst_ref=halo[kind].at[dst, taken, kv_cols(c)],
            send_sem=send_sem.at[kind, dst, c],
            recv_sem=recv_sem.at[kind, dst, c],
            device_id={"seq": device},
            device_id_type=pl.DeviceIdType.MESH,
        )

    def both(act, src, dst, c, taken, device):
        for kind in range(2):
            act(copy_of(kind, src, dst, c, taken, device))

    def start(copy):
        copy.start()

    def sent(copy):
        copy.wait_send()

    def arrived(copy):
        copy.wait_recv()

    def upward(act, c):
        half = (place == 0) | ((place == 2) & (c >= own_first))

        @pl.when(half)
        def _():
            both(act, None, 0, c, lows, above)

        @pl.when(jnp.logical_not(half))
        def _():
            both(act, None, 0, c, whole, above)

    def from_below(act, c):
        half = (place == 0) | ((place == 2) & (c >= below_first))

        @pl.when(half)
        def _():
            both(act, None, 0, c, lows, partner)

        @pl.when(jnp.logical_not(half))
        def _():
            both(act, None, 0, c, whole, partner)

    def over(act, src, c):
        half = (far == 1) & (core == 0) & (c >= below_first)

        @pl.when(half)
        def _():
            both(act, src, 2, c, lows, across)

        @pl.when(jnp.logical_not(half))
        def _():
            both(act, src, 2, c, whole, across)

    def from_over(act, c):
        half = (place == 0) & (c >= below_first)

        @pl.when(half)
        def _():
            both(act, None, 2, c, lows, partner)

        @pl.when(jnp.logical_not(half))
        def _():
            both(act, None, 2, c, whole, partner)

    def cross(kind, spot):
        return pltpu.make_async_remote_copy(
            src_ref=own_hbm[kind].at[tops, kv_cols(own_first + spot)],
            dst_ref=transit[kind].at[spot],
            send_sem=transit_send.at[kind, spot],
            recv_sem=transit_recv.at[kind, spot],
            device_id={"seq": across},
            device_id_type=pl.DeviceIdType.MESH,
        )

    def climb(kind, spot, first):
        return pltpu.make_async_remote_copy(
            src_ref=transit[kind].at[spot],
            dst_ref=halo[kind].at[2, tops, kv_cols(first + spot)],
            send_sem=first_send.at[kind, spot],
            recv_sem=first_recv.at[kind, spot],
            device_id={"seq": above},
            device_id_type=pl.DeviceIdType.MESH,
        )

    barrier = pltpu.get_barrier_semaphore()

    def greet(device):
        pl.semaphore_signal(
            barrier, inc=1, device_id={"seq": device}, device_id_type=pl.DeviceIdType.MESH
        )

    greet(across)

    @pl.when(has_above)
    def _():
        greet(above)

    @pl.when(has_below)
    def _():
        greet(below)

    greet(partner)
    local = [
        pltpu.make_async_copy(k_hbm, k_own, local_sem.at[0]),
        pltpu.make_async_copy(v_hbm, v_own, local_sem.at[1]),
        pltpu.make_async_copy(q_hbm, q_own, local_sem.at[2]),
    ]
    for copy in local:
        copy.start()
    pl.semaphore_wait(barrier, 2 + has_above.astype(jnp.int32) + has_below.astype(jnp.int32))

    def cross_start(spot):
        @pl.when((place == 2) & (spot < chunks - own_first))
        def _():
            for kind in range(2):
                cross(kind, spot).start()

    def first_sends(c, carry):
        @pl.when(far == 0)
        def _():
            over(start, None, c)

        @pl.when(has_above & ((place != 0) | (c < UP_AHEAD)))
        def _():
            upward(start, c)

        @pl.when(c < CROSS_AHEAD)
        def _():
            cross_start(c)

        return carry

    lax.fori_loop(0, chunks, first_sends, 0)

    @pl.when(core == 0)
    def _():
        def give(c, carry):
            both(start, None, 1, c, whole, partner)
            return carry

        lax.fori_loop(0, chunks, give, 0)

    @pl.when(jnp.logical_not(has_below))
    def _():
        for r in range(4):

            @pl.when((r == 0) | (r > place))
            def _():
                def clear(i, carry):
                    taken = pl.ds(pl.multiple_of(i * 16, 16), 16)
                    for ref in halo:
                        ref[r, taken, :] = jnp.zeros((16, kv_width), ref.dtype)
                    return carry

                lax.fori_loop(0, rows // 16, clear, 0)

    def shown(held, first):
        return jnp.concatenate(
            [
                jnp.full((1, BLK), jnp.where(b >= first, 0.0, HIDDEN), jnp.float32)
                for b in held
            ],
            axis=1,
        )

    hide_main = []
    hide_late = []
    for a in range(blocks):
        number = me * blocks + a
        end = jnp.int32(0)
        first = jnp.int32(0)
        for d in range(docs_ref.shape[0]):
            end = end + docs_ref[d]
            first = jnp.where(end <= number, end, first)
        held = [(me - 4) * blocks + b for b in range(a + 1, blocks)]
        for r in (early, 2):
            held += [(me - r) * blocks + b for b in range(blocks)]
        held += [me * blocks + b for b in range(a + 1)]
        hide_main.append(shown(held, first))
        hide_late.append(shown([(me - late) * blocks + b for b in range(blocks)], first))

    for copy in local:
        copy.wait()

    def heads_of(c):
        return [pl.ds(pl.multiple_of((c * ratio + g) * DH, DH), DH) for g in range(ratio)]

    def query_tile(c, a):
        return jnp.concatenate(
            [q_own[a * BLK : (a + 1) * BLK, hc] for hc in heads_of(c)], axis=0
        )

    def dot_keys(q_tile, keys):
        return lax.dot_general(
            q_tile, keys, (((1,), (1,)), ((), ())), preferred_element_type=jnp.float32
        )

    def main_part(c):
        q_index = lax.broadcasted_iota(jnp.int32, (BLK, BLK), 0)
        k_index = lax.broadcasted_iota(jnp.int32, (BLK, BLK), 1)
        causal = jnp.where(k_index <= q_index, 0.0, HIDDEN).astype(jnp.float32)
        causal = jnp.concatenate([causal] * ratio, axis=0)
        cols = kv_cols(c)
        kept = []
        for a in range(blocks):
            own_rows = (a + 1) * BLK

            def gathered(halo_ref, own_ref):
                parts = []
                if own_rows < rows:
                    parts.append(halo_ref[0, own_rows:, cols])
                parts.append(halo_ref[early, :, cols])
                parts.append(halo_ref[2, :, cols])
                parts.append(own_ref[:own_rows, cols])
                return jnp.concatenate(parts, axis=0)

            scores = dot_keys(query_tile(c, a), gathered(k_halo, k_own)) + hide_main[a]
            scores = jnp.concatenate([scores[:, :-BLK], scores[:, -BLK:] + causal], axis=1)
            top = jnp.max(scores, axis=1, keepdims=True)
            weights = jnp.exp2((scores - top) * EXP2_SCALE)
            total = jnp.sum(weights, axis=1, keepdims=True)
            blended = jnp.dot(
                weights.astype(jnp.bfloat16),
                gathered(v_halo, v_own),
                preferred_element_type=jnp.float32,
            )
            kept.append((top, total, blended))
        return kept

    def late_part(c, kept):
        cols = kv_cols(c)
        for a in range(blocks):
            top, total, blended = kept[a]
            scores = dot_keys(query_tile(c, a), k_halo[late, :, cols]) + hide_late[a]
            new_top = jnp.maximum(top, jnp.max(scores, axis=1, keepdims=True))
            shrink = jnp.exp2((top - new_top) * EXP2_SCALE)
            weights = jnp.exp2((scores - new_top) * EXP2_SCALE)
            total = total * shrink + jnp.sum(weights, axis=1, keepdims=True)
            blended = blended * shrink + jnp.dot(
                weights.astype(jnp.bfloat16),
                v_halo[late, :, cols],
                preferred_element_type=jnp.float32,
            )
            blended = (blended / total).astype(o_own.dtype)
            for g, hc in enumerate(heads_of(c)):
                o_own[a * BLK : (a + 1) * BLK, hc] = blended[g * BLK : (g + 1) * BLK]

    def step_of(t, carry):
        @pl.when((t < chunks) & has_below)
        def _():
            from_below(arrived, t)

            @pl.when(far == 1)
            def _():
                over(start, 0, t)

            @pl.when(core == 1)
            def _():
                both(start, 0, 3, t, whole, partner)

        @pl.when(has_above)
        def _():
            cross_start(t + CROSS_AHEAD)

            @pl.when((place == 0) & (t < chunks - own_first))
            def _():
                for kind in range(2):
                    cross(kind, t).wait_recv()
                    climb(kind, t, own_first).start()

            @pl.when((place == 0) & (t + UP_AHEAD < chunks))
            def _():
                upward(start, t + UP_AHEAD)

        @pl.when(t >= 1)
        def _():
            c = t - 1

            @pl.when(has_far)
            def _():
                from_over(arrived, c)

                @pl.when((place == 0) & (c >= below_first))
                def _():
                    for kind in range(2):
                        climb(kind, c - below_first, below_first).wait_recv()

                both(start, 2, 4 - late, c, whole, partner)

            @pl.when((core == 1) | has_below)
            def _():
                both(arrived, None, early, c, whole, partner)

            kept = main_part(c)

            @pl.when(has_far)
            def _():
                both(arrived, None, late, c, whole, partner)

            late_part(c, kept)

        return carry

    lax.fori_loop(0, chunks + 1, step_of, 0)

    def finish(c, carry):
        @pl.when(has_above)
        def _():
            upward(sent, c)

            @pl.when((place == 2) & (c < chunks - own_first))
            def _():
                for kind in range(2):
                    cross(kind, c).wait_send()

            @pl.when((place == 0) & (c < chunks - own_first))
            def _():
                for kind in range(2):
                    climb(kind, c, own_first).wait_send()

        @pl.when((far == 0) | has_below)
        def _():
            over(sent, None, c)

        @pl.when(core == 0)
        def _():
            both(sent, None, 1, c, whole, partner)

        @pl.when((core == 1) & has_below)
        def _():
            both(sent, None, 3, c, whole, partner)

        @pl.when(has_far)
        def _():
            both(sent, None, 4 - late, c, whole, partner)

        return carry

    lax.fori_loop(0, chunks, finish, 0)


def on_paired_device(n, queries, keys, values, doc_blocks):
    rows, kv_width = keys.shape
    chunks = kv_width // DH
    return pl.pallas_call(
        functools.partial(paired_kernel, n),
        out_shape=pltpu.VMEM(queries.shape, queries.dtype),
        in_specs=[pl.BlockSpec(memory_space=pltpu.SMEM)]
        + [pl.BlockSpec(memory_space=pl.ANY)] * 3,
        out_specs=pl.BlockSpec(memory_space=pltpu.VMEM),
        scratch_shapes=[
            pltpu.VMEM(queries.shape, queries.dtype),
            pltpu.VMEM(keys.shape, keys.dtype),
            pltpu.VMEM(values.shape, values.dtype),
            pltpu.VMEM((4, rows, kv_width), keys.dtype),
            pltpu.VMEM((4, rows, kv_width), values.dtype),
            pltpu.VMEM((chunks, BLK, DH), keys.dtype),
            pltpu.VMEM((chunks, BLK, DH), values.dtype),
            pltpu.SemaphoreType.DMA((3,)),
            pltpu.SemaphoreType.DMA((2, 4, chunks)),
            pltpu.SemaphoreType.DMA((2, 4, chunks)),
            pltpu.SemaphoreType.DMA((2, chunks)),
            pltpu.SemaphoreType.DMA((2, chunks)),
            pltpu.SemaphoreType.DMA((2, chunks)),
            pltpu.SemaphoreType.DMA((2, chunks)),
        ],
        compiler_params=pltpu.CompilerParams(
            collective_id=0, has_side_effects=True, vmem_limit_bytes=60 * 1024 * 1024
        ),
    )(doc_blocks, queries, keys, values)


def solution(mesh):
    n = mesh.shape["seq"]
    spread = P(("groups", "seq"), None)
    return jax.shard_map(
        functools.partial(on_paired_device if n // 4 == 4 else on_device, n),
        mesh=mesh,
        in_specs=(spread, spread, spread, P("groups")),
        out_specs=spread,
        check_vma=False,
    )
```

```python
import functools

import jax
import jax.numpy as jnp
from jax import lax
from jax.experimental import pallas as pl
from jax.experimental.pallas import tpu as pltpu
from jax.sharding import PartitionSpec as P

DH = 128
BLK = 128
CHUNK_HEADS = 1
ROUTED = 1
EXP2_SCALE = 144.0 ** (-0.5) * 1.4426950408889634
HIDDEN = -1e30
ROUTED_STEP = 6
CROSS_AHEAD = 4
UP_AHEAD = 3


def kernel(
    n,
    window,
    docs_ref,
    q_hbm,
    k_hbm,
    v_hbm,
    o_own,
    q_own,
    k_own,
    v_own,
    k_halo,
    v_halo,
    local_sem,
    send_sem,
    recv_sem,
    k_transit,
    v_transit,
    transit_send,
    transit_recv,
    forward_send,
):
    me = lax.axis_index("seq")
    pairs = window // 2
    place = lax.rem(me, window)
    base = me - place
    pair = place // 2
    core = lax.rem(me, 2)
    partner = me + 1 - 2 * core
    above = me + window
    below = me - window
    has_above = above < n
    has_below = below >= 0

    rows, kv_width = k_hbm.shape
    ratio = q_hbm.shape[1] // kv_width
    width = CHUNK_HEADS * DH
    chunks = kv_width // width
    blocks = rows // BLK
    own_hbm = (k_hbm, v_hbm)
    halo = (k_halo, v_halo)
    transit = (k_transit, v_transit)
    first_routed = chunks - ROUTED

    def pair_device(step):
        return base + 2 * lax.rem(pair + step, pairs) + core

    def kv_cols(c):
        return pl.ds(pl.multiple_of(c * width, width), width)

    def remote_one(kind, c, src_slot, dst_slot, device, from_row=0):
        taken = pl.ds(from_row, rows - from_row)
        if src_slot is None:
            src = own_hbm[kind].at[taken, kv_cols(c)]
        else:
            src = halo[kind].at[src_slot, taken, kv_cols(c)]
        return pltpu.make_async_remote_copy(
            src_ref=src,
            dst_ref=halo[kind].at[dst_slot, taken, kv_cols(c)],
            send_sem=send_sem.at[kind, dst_slot, c],
            recv_sem=recv_sem.at[kind, dst_slot, c],
            device_id={"seq": device},
            device_id_type=pl.DeviceIdType.MESH,
        )

    def is_routed(c):
        return (c >= first_routed) & (c < first_routed + ROUTED)

    def turn(spot):
        moved = jnp.where(spot < chunks - 1, spot + 1, first_routed - 1)
        return jnp.where((pair == 0) & (spot >= first_routed - 1), moved, spot)

    def across(kind, c, step):
        spot = c - first_routed
        return pltpu.make_async_remote_copy(
            src_ref=own_hbm[kind].at[:, kv_cols(c)],
            dst_ref=transit[kind].at[step - 1, spot],
            send_sem=transit_send.at[kind, step - 1, spot],
            recv_sem=transit_recv.at[kind, step - 1, spot],
            device_id={"seq": pair_device(step)},
            device_id_type=pl.DeviceIdType.MESH,
        )

    def forward(kind, c, step):
        spot = c - first_routed
        return pltpu.make_async_remote_copy(
            src_ref=transit[kind].at[step - 1, spot],
            dst_ref=halo[kind].at[2 * step, :, kv_cols(c)],
            send_sem=forward_send.at[kind, step - 1, spot],
            recv_sem=recv_sem.at[kind, 2 * step, c],
            device_id={"seq": above},
            device_id_type=pl.DeviceIdType.MESH,
        )

    def remote(c, src_slot, dst_slot, device):
        return [remote_one(kind, c, src_slot, dst_slot, device) for kind in range(2)]

    def upward(kind, c, act):
        @pl.when(place == 0)
        def _():
            act(remote_one(kind, c, None, 0, above, BLK))

        @pl.when(place != 0)
        def _():
            act(remote_one(kind, c, None, 0, above))

    def start(copies):
        for copy in copies:
            copy.start()

    def partner_slot(step):
        return lax.rem(2 * step + 1 - 2 * core + window, window)

    barrier = pltpu.get_barrier_semaphore()

    def greet(device):
        pl.semaphore_signal(
            barrier, inc=1, device_id={"seq": device}, device_id_type=pl.DeviceIdType.MESH
        )

    greet(partner)
    for step in range(1, pairs):
        greet(pair_device(step))

    @pl.when(has_above)
    def _():
        greet(above)

    @pl.when(has_below)
    def _():
        greet(below)

    local = [
        pltpu.make_async_copy(k_hbm, k_own, local_sem.at[0]),
        pltpu.make_async_copy(v_hbm, v_own, local_sem.at[1]),
        pltpu.make_async_copy(q_hbm, q_own, local_sem.at[2]),
    ]
    start(local)
    pl.semaphore_wait(
        barrier, pairs + has_above.astype(jnp.int32) + has_below.astype(jnp.int32)
    )

    def cross_first(spot, carry):
        for step in range(1, pairs):

            @pl.when((pair + step >= pairs) & has_above)
            def _():
                for kind in range(2):
                    across(kind, first_routed + spot, step).start()

        return carry

    lax.fori_loop(0, ROUTED, cross_first, 0)

    def first_sends(c, carry):
        @pl.when(has_above)
        def _():
            for kind in range(2):
                upward(kind, c, lambda copy: copy.start())

        for step in range(1, pairs):

            @pl.when(pair + step < pairs)
            def _():
                start(remote(c, None, 2 * step, pair_device(step)))

        @pl.when(core == 0)
        def _():
            start(remote(c, None, 1, partner))

        return carry

    lax.fori_loop(0, chunks, first_sends, 0)

    @pl.when(jnp.logical_not(has_below))
    def _():
        for r in range(window):

            @pl.when((r == 0) | (r > place))
            def _():
                def clear(i, carry):
                    taken = pl.ds(pl.multiple_of(i * 16, 16), 16)
                    for ref in halo:
                        ref[r, taken, :] = jnp.zeros((16, kv_width), ref.dtype)
                    return carry

                lax.fori_loop(0, rows // 16, clear, 0)

    hide_rows = []
    for a in range(blocks):
        number = me * blocks + a
        end = jnp.int32(0)
        first = jnp.int32(0)
        for d in range(docs_ref.shape[0]):
            end = end + docs_ref[d]
            first = jnp.where(end <= number, end, first)
        held = [(me - window) * blocks + b for b in range(a + 1, blocks)]
        for r in range(1, window):
            held += [(me - r) * blocks + b for b in range(blocks)]
        held += [me * blocks + b for b in range(a + 1)]
        hide_rows.append(
            jnp.concatenate(
                [
                    jnp.full((1, BLK), jnp.where(b >= first, 0.0, HIDDEN), jnp.float32)
                    for b in held
                ],
                axis=1,
            )
        )

    for copy in local:
        copy.wait()

    def attend(c):
        q_index = lax.broadcasted_iota(jnp.int32, (BLK, BLK), 0)
        k_index = lax.broadcasted_iota(jnp.int32, (BLK, BLK), 1)
        causal = jnp.where(k_index <= q_index, 0.0, HIDDEN).astype(jnp.float32)
        causal = jnp.concatenate([causal] * ratio, axis=0)
        for h in range(CHUNK_HEADS):
            cols = pl.ds(pl.multiple_of(c * width + h * DH, DH), DH)
            for a in range(blocks):
                own_rows = (a + 1) * BLK

                def gathered(halo_ref, own_ref):
                    parts = []
                    if own_rows < rows:
                        parts.append(halo_ref[0, own_rows:, cols])
                    for r in range(1, window):
                        parts.append(halo_ref[r, :, cols])
                    parts.append(own_ref[:own_rows, cols])
                    return jnp.concatenate(parts, axis=0)

                head_cols = [
                    pl.ds(pl.multiple_of((c * width + h * DH) * ratio + g * DH, DH), DH)
                    for g in range(ratio)
                ]
                tile_rows = slice(a * BLK, (a + 1) * BLK)
                q_tile = jnp.concatenate([q_own[tile_rows, hc] for hc in head_cols], axis=0)
                scores = lax.dot_general(
                    q_tile,
                    gathered(k_halo, k_own),
                    (((1,), (1,)), ((), ())),
                    preferred_element_type=jnp.float32,
                )
                scores = scores + hide_rows[a]
                scores = jnp.concatenate([scores[:, :-BLK], scores[:, -BLK:] + causal], axis=1)
                top = jnp.max(scores, axis=1, keepdims=True)
                weights = jnp.exp2((scores - top) * EXP2_SCALE)
                total = jnp.sum(weights, axis=1, keepdims=True)
                blended = jnp.dot(
                    weights.astype(jnp.bfloat16),
                    gathered(v_halo, v_own),
                    preferred_element_type=jnp.float32,
                )
                blended = (blended / total).astype(o_own.dtype)
                for g in range(ratio):
                    o_own[tile_rows, head_cols[g]] = blended[g * BLK : (g + 1) * BLK]

    def arrived(c, slot):
        for copy in remote(c, None, slot, partner):
            copy.wait_recv()

    def step_of(t, carry):
        @pl.when((t < chunks) & has_below)
        def _():
            c = t
            for kind in range(2):
                upward(kind, c, lambda copy: copy.wait_recv())

                @pl.when(core == 1)
                def _():
                    remote_one(kind, c, 0, window - 1, partner).start()

                for step in range(1, pairs):

                    @pl.when((pair + step >= pairs) & jnp.logical_not(is_routed(c)))
                    def _():
                        remote_one(kind, c, 0, 2 * step, pair_device(step)).start()

        @pl.when((t < ROUTED) & has_above)
        def _():
            for step in range(1, pairs):

                @pl.when(step > pair)
                def _():
                    for kind in range(2):
                        across(kind, t + first_routed, step).wait_recv()
                        forward(kind, t + first_routed, step).start()

        @pl.when((t >= 1) & (t < chunks + 1))
        def _():
            c = turn(t - 1)
            for step in range(1, pairs):

                @pl.when((pair >= step) | has_below)
                def _():
                    for kind in range(2):
                        remote_one(kind, c, None, 2 * step, partner).wait_recv()
                        remote_one(kind, c, 2 * step, partner_slot(step), partner).start()

        @pl.when((t >= 2) & (t < chunks + 2))
        def _():
            c = turn(t - 2)
            for r in range(1, window, 2):

                @pl.when((place >= r) | has_below)
                def _():
                    arrived(c, r)

            attend(c)

        return carry

    lax.fori_loop(0, chunks + 2, step_of, 0)

    def finish(c, carry):
        def sent(slot):
            for copy in remote(c, None, slot, partner):
                copy.wait_send()

        @pl.when(has_above)
        def _():
            for kind in range(2):
                upward(kind, c, lambda copy: copy.wait_send())

        @pl.when((core == 0) | has_below)
        def _():
            sent(partner_slot(0))

        for step in range(1, pairs):

            @pl.when((pair + step < pairs) | (has_below & jnp.logical_not(is_routed(c))))
            def _():
                sent(2 * step)

            @pl.when((pair + step >= pairs) & has_above & is_routed(c))
            def _():
                for kind in range(2):
                    across(kind, c, step).wait_send()

            @pl.when((step > pair) & has_above & is_routed(c))
            def _():
                for kind in range(2):
                    forward(kind, c, step).wait_send()

            @pl.when((pair >= step) | has_below)
            def _():
                sent(partner_slot(step))

        return carry

    lax.fori_loop(0, chunks, finish, 0)


def on_device(n, queries, keys, values, doc_blocks):
    window = n // 4
    rows, kv_width = keys.shape
    chunks = kv_width // (CHUNK_HEADS * DH)
    return pl.pallas_call(
        functools.partial(kernel, n, window),
        out_shape=pltpu.VMEM(queries.shape, queries.dtype),
        in_specs=[pl.BlockSpec(memory_space=pltpu.SMEM)]
        + [pl.BlockSpec(memory_space=pl.ANY)] * 3,
        out_specs=pl.BlockSpec(memory_space=pltpu.VMEM),
        scratch_shapes=[
            pltpu.VMEM(queries.shape, queries.dtype),
            pltpu.VMEM(keys.shape, keys.dtype),
            pltpu.VMEM(values.shape, values.dtype),
            pltpu.VMEM((window, rows, kv_width), keys.dtype),
            pltpu.VMEM((window, rows, kv_width), values.dtype),
            pltpu.SemaphoreType.DMA((3,)),
            pltpu.SemaphoreType.DMA((2, window, chunks)),
            pltpu.SemaphoreType.DMA((2, window, chunks)),
            pltpu.VMEM((window // 2 - 1, ROUTED, rows, CHUNK_HEADS * DH), keys.dtype),
            pltpu.VMEM((window // 2 - 1, ROUTED, rows, CHUNK_HEADS * DH), values.dtype),
            pltpu.SemaphoreType.DMA((2, window // 2 - 1, ROUTED)),
            pltpu.SemaphoreType.DMA((2, window // 2 - 1, ROUTED)),
            pltpu.SemaphoreType.DMA((2, window // 2 - 1, ROUTED)),
        ],
        compiler_params=pltpu.CompilerParams(
            collective_id=0, has_side_effects=True, vmem_limit_bytes=60 * 1024 * 1024
        ),
    )(doc_blocks, queries, keys, values)


UP, OVER, CROSS, CLIMB, GIFT, RISE, LATE, EXTRA = range(8)


def paired_kernel(
    n,
    docs_hbm,
    q_hbm,
    k_hbm,
    v_hbm,
    o_own,
    q_own,
    own,
    halo,
    transit,
    docs_ref,
    local_sem,
    z_recv,
    y_recv,
    pair_recv,
    cross_recv,
    gift_recv,
    rise_recv,
    send_sem,
):
    me = lax.axis_index("seq")
    place = lax.rem(me, 4)
    row = me // 4
    last_row = n // 4 - 1
    far = place // 2
    core = lax.rem(me, 2)
    partner = me + 1 - 2 * core
    across = me + 2 - 4 * far
    above = me + 4
    below = me - 4
    has_above = above < n
    has_below = below >= 0

    rows, kv_width = k_hbm.shape
    ratio = q_hbm.shape[1] // kv_width
    chunks = kv_width // DH
    last = chunks - 1
    blocks = rows // BLK
    early = jnp.where(core == 0, 3, 1)
    late = 4 - early
    has_far = (far == 1) | has_below
    tops = slice(0, BLK)
    lows = slice(BLK, rows)
    whole = slice(0, rows)

    def routed(of_row):
        return jnp.minimum(chunks, ROUTED_STEP * (last_row - of_row))

    own_first = chunks - routed(row)
    below_first = chunks - routed(row - 1)

    def kv_cols(c, count=1):
        return pl.ds(pl.multiple_of(c * DH, DH), count * DH)

    def remote(src, dst, out, into, device):
        return pltpu.make_async_remote_copy(
            src_ref=src,
            dst_ref=dst,
            send_sem=send_sem.at[out],
            recv_sem=into,
            device_id={"seq": device},
            device_id_type=pl.DeviceIdType.MESH,
        )

    def send_own(slot, c, taken, out, into, device):
        for kind, hbm in enumerate((k_hbm, v_hbm)):
            remote(
                hbm.at[taken, kv_cols(c)],
                halo.at[kind, slot, taken, kv_cols(c)],
                out,
                into,
                device,
            ).start()

    def send_held(src, dst, c, taken, out, into, device):
        remote(
            halo.at[:, src, taken, kv_cols(c)],
            halo.at[:, dst, taken, kv_cols(c)],
            out,
            into,
            device,
        ).start()

    def landed(ref, sem):
        pltpu.make_async_copy(ref, ref, sem).wait()

    def chunk_of(slot, c, taken=whole):
        return halo.at[:, slot, taken, kv_cols(c)]

    def by_half(half, act):
        @pl.when(half)
        def _():
            act(lows)

        @pl.when(jnp.logical_not(half))
        def _():
            act(whole)

    def upward(c):
        half = (place == 0) | ((place == 2) & (c >= own_first))
        by_half(half, lambda taken: send_own(0, c, taken, UP, z_recv.at[c], above))

    def cross_start(c):
        for kind, hbm in enumerate((k_hbm, v_hbm)):
            remote(
                hbm.at[tops, kv_cols(c)],
                transit.at[kind, :, kv_cols(c)],
                CROSS,
                cross_recv.at[c // 2],
                across,
            ).start()

    def climb_start(c):
        remote(
            transit.at[:, :, kv_cols(c)],
            halo.at[:, 2, tops, kv_cols(c)],
            CLIMB,
            y_recv.at[c],
            above,
        ).start()

    barrier = pltpu.get_barrier_semaphore()

    def greet(device):
        pl.semaphore_signal(
            barrier, inc=1, device_id={"seq": device}, device_id_type=pl.DeviceIdType.MESH
        )

    greet(across)

    @pl.when(has_above)
    def _():
        greet(above)

    @pl.when(has_below)
    def _():
        greet(below)

    greet(partner)
    local = [
        pltpu.make_async_copy(k_hbm, own.at[0], local_sem.at[0]),
        pltpu.make_async_copy(v_hbm, own.at[1], local_sem.at[1]),
        pltpu.make_async_copy(q_hbm, q_own, local_sem.at[2]),
    ]
    docs = pltpu.make_async_copy(docs_hbm, docs_ref, local_sem.at[3])
    docs.start()
    for copy in local:
        copy.start()
    pl.semaphore_wait(barrier, 2 + has_above.astype(jnp.int32) + has_below.astype(jnp.int32))

    def first_sends(c, carry):
        @pl.when((place == 1) | ((place == 0) & (c < last)))
        def _():
            send_own(2, c, whole, OVER, y_recv.at[c], across)

        @pl.when(has_above & ((place != 0) | (c < UP_AHEAD)))
        def _():
            upward(c)

        @pl.when((place == 2) & (c < CROSS_AHEAD) & (own_first + c < chunks))
        def _():
            cross_start(own_first + c)

        @pl.when(core == 0)
        def _():
            given = last - c
            send_own(1, given, whole, GIFT, gift_recv.at[(given + 1) // chunks], partner)

        return carry

    lax.fori_loop(0, chunks, first_sends, 0)

    @pl.when(core == 1)
    def _():
        landed(chunk_of(1, last), gift_recv.at[1])

        @pl.when(far == 0)
        def _():
            send_held(1, 3, last, whole, EXTRA, pair_recv.at[last], across)

    @pl.when(jnp.logical_not(has_below))
    def _():
        for r in range(4):

            @pl.when((r == 0) | (r > place))
            def _():
                def clear(i, carry):
                    taken = pl.ds(pl.multiple_of(i * 16, 16), 16)
                    for kind in range(2):
                        halo[kind, r, taken, :] = jnp.zeros((16, kv_width), halo.dtype)
                    return carry

                lax.fori_loop(0, rows // 16, clear, 0)

    def shown(held, first):
        return jnp.concatenate(
            [
                jnp.full((1, BLK), jnp.where(b >= first, 0.0, HIDDEN), jnp.float32)
                for b in held
            ],
            axis=1,
        )

    docs.wait()
    second = jnp.where(place == 2, 1, 2)
    third = jnp.where(place == 2, 2, late)

    def slot_blocks(r):
        return [(me - r) * blocks + b for b in range(blocks)]

    hide_all = []
    hide_main = []
    hide_second = []
    hide_third = []
    for a in range(blocks):
        number = me * blocks + a
        end = jnp.int32(0)
        first = jnp.int32(0)
        for d in range(docs_ref.shape[0]):
            end = end + docs_ref[d]
            first = jnp.where(end <= number, end, first)
        oldest = slot_blocks(4)[a + 1 :]
        mine = slot_blocks(0)[: a + 1]
        between = slot_blocks(3) + slot_blocks(2) + slot_blocks(1)
        hide_all.append(shown(oldest + between + mine, first))
        hide_main.append(shown(oldest + slot_blocks(early) + mine, first))
        hide_second.append(shown(slot_blocks(second), first))
        hide_third.append(shown(slot_blocks(third), first))

    for copy in local:
        copy.wait()

    def heads_of(c):
        return [pl.ds(pl.multiple_of((c * ratio + g) * DH, DH), DH) for g in range(ratio)]

    def query_tile(c, a):
        return jnp.concatenate(
            [q_own[a * BLK : (a + 1) * BLK, hc] for hc in heads_of(c)], axis=0
        )

    def dot_keys(q_tile, keys):
        return lax.dot_general(
            q_tile, keys, (((1,), (1,)), ((), ())), preferred_element_type=jnp.float32
        )

    def gathered(kind, a, slots, cols):
        parts = []
        if a + 1 < blocks:
            parts.append(halo[kind, 0, (a + 1) * BLK :, cols])
        for r in slots:
            parts.append(halo[kind, r, :, cols])
        parts.append(own[kind, : (a + 1) * BLK, cols])
        return jnp.concatenate(parts, axis=0)

    def attend(c, slots, hide):
        q_index = lax.broadcasted_iota(jnp.int32, (BLK, BLK), 0)
        k_index = lax.broadcasted_iota(jnp.int32, (BLK, BLK), 1)
        causal = jnp.where(k_index <= q_index, 0.0, HIDDEN).astype(jnp.float32)
        causal = jnp.concatenate([causal] * ratio, axis=0)
        cols = kv_cols(c)
        kept = []
        for a in range(blocks):
            scores = dot_keys(query_tile(c, a), gathered(0, a, slots, cols)) + hide[a]
            scores = jnp.concatenate([scores[:, :-BLK], scores[:, -BLK:] + causal], axis=1)
            top = jnp.max(scores, axis=1, keepdims=True)
            weights = jnp.exp2((scores - top) * EXP2_SCALE)
            total = jnp.sum(weights, axis=1, keepdims=True)
            blended = jnp.dot(
                weights.astype(jnp.bfloat16),
                gathered(1, a, slots, cols),
                preferred_element_type=jnp.float32,
            )
            kept.append((top, total, blended))
        return kept

    def store(c, kept):
        for a in range(blocks):
            top, total, blended = kept[a]
            blended = (blended / total).astype(o_own.dtype)
            for g, hc in enumerate(heads_of(c)):
                o_own[a * BLK : (a + 1) * BLK, hc] = blended[g * BLK : (g + 1) * BLK]

    def merge(slot, hide, kept):
        merged = []
        cols = kv_cols(last)
        for a in range(blocks):
            top, total, blended = kept[a]
            scores = dot_keys(query_tile(last, a), halo[0, slot, :, cols]) + hide[a]
            new_top = jnp.maximum(top, jnp.max(scores, axis=1, keepdims=True))
            shrink = jnp.exp2((top - new_top) * EXP2_SCALE)
            weights = jnp.exp2((scores - new_top) * EXP2_SCALE)
            total = total * shrink + jnp.sum(weights, axis=1, keepdims=True)
            blended = blended * shrink + jnp.dot(
                weights.astype(jnp.bfloat16),
                halo[1, slot, :, cols],
                preferred_element_type=jnp.float32,
            )
            merged.append((new_top, total, blended))
        return merged

    def z_part(t):
        @pl.when(has_below)
        def _():
            half = (place == 0) | ((place == 2) & (t >= below_first))
            by_half(half, lambda taken: landed(chunk_of(0, t, taken), z_recv.at[t]))

            @pl.when(far == 1)
            def _():
                half = (core == 0) & (t >= below_first)
                by_half(
                    half,
                    lambda taken: send_held(0, 2, t, taken, OVER, y_recv.at[t], across),
                )

            @pl.when((core == 1) & (t < last))
            def _():
                send_held(0, 3, t, whole, RISE, pair_recv.at[t], partner)

            @pl.when((core == 1) & (t == last))
            def _():
                send_held(0, 3, t, whole, RISE, rise_recv.at[0], partner)

        @pl.when(has_above)
        def _():
            ahead = own_first + t + CROSS_AHEAD

            @pl.when((place == 2) & (ahead < chunks))
            def _():
                cross_start(ahead)

            @pl.when((place == 0) & (own_first + t < chunks) & (lax.rem(t, 2) == 0))
            def _():
                c = own_first + t
                landed(transit.at[:, :, kv_cols(c, 2)], cross_recv.at[c // 2])
                climb_start(c)
                climb_start(c + 1)

            @pl.when((place == 0) & (t + UP_AHEAD < chunks))
            def _():
                upward(t + UP_AHEAD)

    def y_part(c):
        @pl.when(has_far)
        def _():
            landed(chunk_of(2, c), y_recv.at[c])
            send_held(2, 4 - late, c, whole, LATE, pair_recv.at[c], partner)

    def attend_all(c):
        both = (core == 0) & has_below

        @pl.when(both)
        def _():
            landed(halo.at[:, 0:2, :, kv_cols(c)], pair_recv.at[c])

        @pl.when(has_far & jnp.logical_not(both))
        def _():
            landed(chunk_of(late, c), pair_recv.at[c])

        store(c, attend(c, (3, 2, 1), hide_all))

    def step_of(t, carry):
        z_part(t)

        @pl.when((t == 2) & (core == 1))
        def _():
            landed(halo.at[:, 1, :, kv_cols(0, last)], gift_recv.at[0])

        @pl.when(t >= 2)
        def _():
            attend_all(t - 2)

        @pl.when(t >= 1)
        def _():
            y_part(t - 1)

        return carry

    lax.fori_loop(0, last, step_of, 0)
    z_part(last)
    attend_all(last - 2)

    @pl.when((core == 0) & has_below)
    def _():
        landed(chunk_of(3, last), rise_recv.at[0])

    kept = attend(last, (early,), hide_main)
    y_part(last - 1)
    attend_all(last - 1)

    @pl.when(has_far & (place != 2))
    def _():
        landed(chunk_of(2, last), y_recv.at[last])
        send_held(2, 4 - late, last, whole, LATE, pair_recv.at[last], partner)

    @pl.when(place == 2)
    def _():
        landed(chunk_of(1, last), pair_recv.at[last])

    kept = merge(second, hide_second, kept)

    @pl.when(has_far & (place != 2))
    def _():
        landed(chunk_of(late, last), pair_recv.at[last])

        @pl.when(place == 3)
        def _():
            send_held(3, 2, last, whole, EXTRA, y_recv.at[last], partner)

    @pl.when(place == 2)
    def _():
        landed(chunk_of(2, last), y_recv.at[last])

    store(last, merge(third, hide_third, kept))

    def drained(taken, width, out):
        landed(halo.at[:, 0, taken, 0:width], send_sem.at[out])

    @pl.when(has_above & (place == 0))
    def _():
        drained(lows, kv_width, UP)

    @pl.when(has_above & (core == 1))
    def _():
        drained(whole, kv_width, UP)

    @pl.when((place == 1) | ((place == 3) & has_below))
    def _():
        drained(whole, kv_width, OVER)

    @pl.when(place == 0)
    def _():
        drained(whole, last * DH, OVER)

    for r in range(last_row):
        count = min(chunks, ROUTED_STEP * (last_row - r))

        @pl.when((place == 2) & (row == r))
        def _():
            drained(whole, (2 * chunks - count) * DH // 2, UP)
            drained(tops, count * DH, CROSS)

        @pl.when((place == 2) & (row == r + 1))
        def _():
            drained(whole, (2 * chunks - count) * DH // 2, OVER)

        @pl.when((place == 0) & (row == r))
        def _():
            drained(tops, count * DH, CLIMB)

    @pl.when(core == 0)
    def _():
        drained(whole, kv_width, GIFT)

    @pl.when((core == 1) & has_below)
    def _():
        drained(whole, kv_width, RISE)

    @pl.when(has_far & (place != 2))
    def _():
        drained(whole, kv_width, LATE)

    @pl.when(place == 2)
    def _():
        drained(whole, last * DH, LATE)

    @pl.when(core == 1)
    def _():
        drained(whole, DH, EXTRA)


def on_paired_device(n, queries, keys, values, doc_blocks):
    rows, kv_width = keys.shape
    chunks = kv_width // DH
    return pl.pallas_call(
        functools.partial(paired_kernel, n),
        out_shape=pltpu.VMEM(queries.shape, queries.dtype),
        in_specs=[pl.BlockSpec(memory_space=pl.ANY)] * 4,
        out_specs=pl.BlockSpec(memory_space=pltpu.VMEM),
        scratch_shapes=[
            pltpu.VMEM(queries.shape, queries.dtype),
            pltpu.VMEM((2, rows, kv_width), keys.dtype),
            pltpu.VMEM((2, 4, rows, kv_width), keys.dtype),
            pltpu.VMEM((2, BLK, kv_width), keys.dtype),
            pltpu.SMEM(doc_blocks.shape, doc_blocks.dtype),
            pltpu.SemaphoreType.DMA((4,)),
            pltpu.SemaphoreType.DMA((chunks,)),
            pltpu.SemaphoreType.DMA((chunks,)),
            pltpu.SemaphoreType.DMA((chunks,)),
            pltpu.SemaphoreType.DMA((chunks // 2,)),
            pltpu.SemaphoreType.DMA((2,)),
            pltpu.SemaphoreType.DMA((1,)),
            pltpu.SemaphoreType.DMA((8,)),
        ],
        compiler_params=pltpu.CompilerParams(
            collective_id=0, has_side_effects=True, vmem_limit_bytes=60 * 1024 * 1024
        ),
    )(doc_blocks, queries, keys, values)


def solution(mesh):
    n = mesh.shape["seq"]
    spread = P(("groups", "seq"), None)
    return jax.shard_map(
        functools.partial(on_paired_device if n // 4 == 4 else on_device, n),
        mesh=mesh,
        in_specs=(spread, spread, spread, P("groups")),
        out_specs=spread,
        check_vma=False,
    )
```

```python
import functools

import jax
import jax.numpy as jnp
from jax import lax
from jax.experimental import pallas as pl
from jax.experimental.pallas import tpu as pltpu
from jax.sharding import PartitionSpec as P

DH = 128
BLK = 128
CHUNK_HEADS = 1
ROUTED = 1
EXP2_SCALE = 144.0 ** (-0.5) * 1.4426950408889634
HIDDEN = -1e30
ROUTED_STEP = 4
ROUTED_BASE = 0
ROUTED_SPARE = 2
CROSS_AHEAD = 4
UP_AHEAD = 3
Z_LEAD = 1


def kernel(
    n,
    window,
    docs_ref,
    q_hbm,
    k_hbm,
    v_hbm,
    o_own,
    q_own,
    k_own,
    v_own,
    k_halo,
    v_halo,
    local_sem,
    send_sem,
    recv_sem,
    k_transit,
    v_transit,
    transit_send,
    transit_recv,
    forward_send,
):
    me = lax.axis_index("seq")
    pairs = window // 2
    place = lax.rem(me, window)
    base = me - place
    pair = place // 2
    core = lax.rem(me, 2)
    partner = me + 1 - 2 * core
    above = me + window
    below = me - window
    has_above = above < n
    has_below = below >= 0

    rows, kv_width = k_hbm.shape
    ratio = q_hbm.shape[1] // kv_width
    width = CHUNK_HEADS * DH
    chunks = kv_width // width
    blocks = rows // BLK
    own_hbm = (k_hbm, v_hbm)
    halo = (k_halo, v_halo)
    transit = (k_transit, v_transit)
    first_routed = chunks - ROUTED

    def pair_device(step):
        return base + 2 * lax.rem(pair + step, pairs) + core

    def kv_cols(c):
        return pl.ds(pl.multiple_of(c * width, width), width)

    def remote_one(kind, c, src_slot, dst_slot, device, from_row=0):
        taken = pl.ds(from_row, rows - from_row)
        if src_slot is None:
            src = own_hbm[kind].at[taken, kv_cols(c)]
        else:
            src = halo[kind].at[src_slot, taken, kv_cols(c)]
        return pltpu.make_async_remote_copy(
            src_ref=src,
            dst_ref=halo[kind].at[dst_slot, taken, kv_cols(c)],
            send_sem=send_sem.at[kind, dst_slot, c],
            recv_sem=recv_sem.at[kind, dst_slot, c],
            device_id={"seq": device},
            device_id_type=pl.DeviceIdType.MESH,
        )

    def is_routed(c):
        return (c >= first_routed) & (c < first_routed + ROUTED)

    def turn(spot):
        moved = jnp.where(spot < chunks - 1, spot + 1, first_routed - 1)
        return jnp.where((pair == 0) & (spot >= first_routed - 1), moved, spot)

    def across(kind, c, step):
        spot = c - first_routed
        return pltpu.make_async_remote_copy(
            src_ref=own_hbm[kind].at[:, kv_cols(c)],
            dst_ref=transit[kind].at[step - 1, spot],
            send_sem=transit_send.at[kind, step - 1, spot],
            recv_sem=transit_recv.at[kind, step - 1, spot],
            device_id={"seq": pair_device(step)},
            device_id_type=pl.DeviceIdType.MESH,
        )

    def forward(kind, c, step):
        spot = c - first_routed
        return pltpu.make_async_remote_copy(
            src_ref=transit[kind].at[step - 1, spot],
            dst_ref=halo[kind].at[2 * step, :, kv_cols(c)],
            send_sem=forward_send.at[kind, step - 1, spot],
            recv_sem=recv_sem.at[kind, 2 * step, c],
            device_id={"seq": above},
            device_id_type=pl.DeviceIdType.MESH,
        )

    def remote(c, src_slot, dst_slot, device):
        return [remote_one(kind, c, src_slot, dst_slot, device) for kind in range(2)]

    def upward(kind, c, act):
        @pl.when(place == 0)
        def _():
            act(remote_one(kind, c, None, 0, above, BLK))

        @pl.when(place != 0)
        def _():
            act(remote_one(kind, c, None, 0, above))

    def start(copies):
        for copy in copies:
            copy.start()

    def partner_slot(step):
        return lax.rem(2 * step + 1 - 2 * core + window, window)

    barrier = pltpu.get_barrier_semaphore()

    def greet(device):
        pl.semaphore_signal(
            barrier, inc=1, device_id={"seq": device}, device_id_type=pl.DeviceIdType.MESH
        )

    greet(partner)
    for step in range(1, pairs):
        greet(pair_device(step))

    @pl.when(has_above)
    def _():
        greet(above)

    @pl.when(has_below)
    def _():
        greet(below)

    local = [
        pltpu.make_async_copy(k_hbm, k_own, local_sem.at[0]),
        pltpu.make_async_copy(v_hbm, v_own, local_sem.at[1]),
        pltpu.make_async_copy(q_hbm, q_own, local_sem.at[2]),
    ]
    start(local)
    pl.semaphore_wait(
        barrier, pairs + has_above.astype(jnp.int32) + has_below.astype(jnp.int32)
    )

    def cross_first(spot, carry):
        for step in range(1, pairs):

            @pl.when((pair + step >= pairs) & has_above)
            def _():
                for kind in range(2):
                    across(kind, first_routed + spot, step).start()

        return carry

    lax.fori_loop(0, ROUTED, cross_first, 0)

    def first_sends(c, carry):
        @pl.when(has_above)
        def _():
            for kind in range(2):
                upward(kind, c, lambda copy: copy.start())

        for step in range(1, pairs):

            @pl.when(pair + step < pairs)
            def _():
                start(remote(c, None, 2 * step, pair_device(step)))

        @pl.when(core == 0)
        def _():
            start(remote(c, None, 1, partner))

        return carry

    lax.fori_loop(0, chunks, first_sends, 0)

    @pl.when(jnp.logical_not(has_below))
    def _():
        for r in range(window):

            @pl.when((r == 0) | (r > place))
            def _():
                def clear(i, carry):
                    taken = pl.ds(pl.multiple_of(i * 16, 16), 16)
                    for ref in halo:
                        ref[r, taken, :] = jnp.zeros((16, kv_width), ref.dtype)
                    return carry

                lax.fori_loop(0, rows // 16, clear, 0)

    hide_rows = []
    for a in range(blocks):
        number = me * blocks + a
        end = jnp.int32(0)
        first = jnp.int32(0)
        for d in range(docs_ref.shape[0]):
            end = end + docs_ref[d]
            first = jnp.where(end <= number, end, first)
        held = [(me - window) * blocks + b for b in range(a + 1, blocks)]
        for r in range(1, window):
            held += [(me - r) * blocks + b for b in range(blocks)]
        held += [me * blocks + b for b in range(a + 1)]
        hide_rows.append(
            jnp.concatenate(
                [
                    jnp.full((1, BLK), jnp.where(b >= first, 0.0, HIDDEN), jnp.float32)
                    for b in held
                ],
                axis=1,
            )
        )

    for copy in local:
        copy.wait()

    def attend(c):
        q_index = lax.broadcasted_iota(jnp.int32, (BLK, BLK), 0)
        k_index = lax.broadcasted_iota(jnp.int32, (BLK, BLK), 1)
        causal = jnp.where(k_index <= q_index, 0.0, HIDDEN).astype(jnp.float32)
        causal = jnp.concatenate([causal] * ratio, axis=0)
        for h in range(CHUNK_HEADS):
            cols = pl.ds(pl.multiple_of(c * width + h * DH, DH), DH)
            for a in range(blocks):
                own_rows = (a + 1) * BLK

                def gathered(halo_ref, own_ref):
                    parts = []
                    if own_rows < rows:
                        parts.append(halo_ref[0, own_rows:, cols])
                    for r in range(1, window):
                        parts.append(halo_ref[r, :, cols])
                    parts.append(own_ref[:own_rows, cols])
                    return jnp.concatenate(parts, axis=0)

                head_cols = [
                    pl.ds(pl.multiple_of((c * width + h * DH) * ratio + g * DH, DH), DH)
                    for g in range(ratio)
                ]
                tile_rows = slice(a * BLK, (a + 1) * BLK)
                q_tile = jnp.concatenate([q_own[tile_rows, hc] for hc in head_cols], axis=0)
                scores = lax.dot_general(
                    q_tile,
                    gathered(k_halo, k_own),
                    (((1,), (1,)), ((), ())),
                    preferred_element_type=jnp.float32,
                )
                scores = scores + hide_rows[a]
                scores = jnp.concatenate([scores[:, :-BLK], scores[:, -BLK:] + causal], axis=1)
                top = jnp.max(scores, axis=1, keepdims=True)
                weights = jnp.exp2((scores - top) * EXP2_SCALE)
                total = jnp.sum(weights, axis=1, keepdims=True)
                blended = jnp.dot(
                    weights.astype(jnp.bfloat16),
                    gathered(v_halo, v_own),
                    preferred_element_type=jnp.float32,
                )
                blended = (blended / total).astype(o_own.dtype)
                for g in range(ratio):
                    o_own[tile_rows, head_cols[g]] = blended[g * BLK : (g + 1) * BLK]

    def arrived(c, slot):
        for copy in remote(c, None, slot, partner):
            copy.wait_recv()

    def step_of(t, carry):
        @pl.when((t < chunks) & has_below)
        def _():
            c = t
            for kind in range(2):
                upward(kind, c, lambda copy: copy.wait_recv())

                @pl.when(core == 1)
                def _():
                    remote_one(kind, c, 0, window - 1, partner).start()

                for step in range(1, pairs):

                    @pl.when((pair + step >= pairs) & jnp.logical_not(is_routed(c)))
                    def _():
                        remote_one(kind, c, 0, 2 * step, pair_device(step)).start()

        @pl.when((t < ROUTED) & has_above)
        def _():
            for step in range(1, pairs):

                @pl.when(step > pair)
                def _():
                    for kind in range(2):
                        across(kind, t + first_routed, step).wait_recv()
                        forward(kind, t + first_routed, step).start()

        @pl.when((t >= 1) & (t < chunks + 1))
        def _():
            c = turn(t - 1)
            for step in range(1, pairs):

                @pl.when((pair >= step) | has_below)
                def _():
                    for kind in range(2):
                        remote_one(kind, c, None, 2 * step, partner).wait_recv()
                        remote_one(kind, c, 2 * step, partner_slot(step), partner).start()

        @pl.when((t >= 2) & (t < chunks + 2))
        def _():
            c = turn(t - 2)
            for r in range(1, window, 2):

                @pl.when((place >= r) | has_below)
                def _():
                    arrived(c, r)

            attend(c)

        return carry

    lax.fori_loop(0, chunks + 2, step_of, 0)

    def finish(c, carry):
        def sent(slot):
            for copy in remote(c, None, slot, partner):
                copy.wait_send()

        @pl.when(has_above)
        def _():
            for kind in range(2):
                upward(kind, c, lambda copy: copy.wait_send())

        @pl.when((core == 0) | has_below)
        def _():
            sent(partner_slot(0))

        for step in range(1, pairs):

            @pl.when((pair + step < pairs) | (has_below & jnp.logical_not(is_routed(c))))
            def _():
                sent(2 * step)

            @pl.when((pair + step >= pairs) & has_above & is_routed(c))
            def _():
                for kind in range(2):
                    across(kind, c, step).wait_send()

            @pl.when((step > pair) & has_above & is_routed(c))
            def _():
                for kind in range(2):
                    forward(kind, c, step).wait_send()

            @pl.when((pair >= step) | has_below)
            def _():
                sent(partner_slot(step))

        return carry

    lax.fori_loop(0, chunks, finish, 0)


def on_device(n, queries, keys, values, doc_blocks):
    window = n // 4
    rows, kv_width = keys.shape
    chunks = kv_width // (CHUNK_HEADS * DH)
    return pl.pallas_call(
        functools.partial(kernel, n, window),
        out_shape=pltpu.VMEM(queries.shape, queries.dtype),
        in_specs=[pl.BlockSpec(memory_space=pltpu.SMEM)]
        + [pl.BlockSpec(memory_space=pl.ANY)] * 3,
        out_specs=pl.BlockSpec(memory_space=pltpu.VMEM),
        scratch_shapes=[
            pltpu.VMEM(queries.shape, queries.dtype),
            pltpu.VMEM(keys.shape, keys.dtype),
            pltpu.VMEM(values.shape, values.dtype),
            pltpu.VMEM((window, rows, kv_width), keys.dtype),
            pltpu.VMEM((window, rows, kv_width), values.dtype),
            pltpu.SemaphoreType.DMA((3,)),
            pltpu.SemaphoreType.DMA((2, window, chunks)),
            pltpu.SemaphoreType.DMA((2, window, chunks)),
            pltpu.VMEM((window // 2 - 1, ROUTED, rows, CHUNK_HEADS * DH), keys.dtype),
            pltpu.VMEM((window // 2 - 1, ROUTED, rows, CHUNK_HEADS * DH), values.dtype),
            pltpu.SemaphoreType.DMA((2, window // 2 - 1, ROUTED)),
            pltpu.SemaphoreType.DMA((2, window // 2 - 1, ROUTED)),
            pltpu.SemaphoreType.DMA((2, window // 2 - 1, ROUTED)),
        ],
        compiler_params=pltpu.CompilerParams(
            collective_id=0, has_side_effects=True, vmem_limit_bytes=60 * 1024 * 1024
        ),
    )(doc_blocks, queries, keys, values)


UP, OVER, CROSS, CLIMB, GIFT, RISE, LATE, EXTRA = range(8)


def paired_kernel(
    n,
    docs_hbm,
    q_hbm,
    k_hbm,
    v_hbm,
    o_own,
    q_own,
    own,
    halo,
    transit,
    docs_ref,
    local_sem,
    z_recv,
    y_recv,
    pair_recv,
    cross_recv,
    gift_recv,
    rise_recv,
    send_sem,
):
    me = lax.axis_index("seq")
    place = lax.rem(me, 4)
    row = me // 4
    last_row = n // 4 - 1
    far = place // 2
    core = lax.rem(me, 2)
    partner = me + 1 - 2 * core
    across = me + 2 - 4 * far
    above = me + 4
    below = me - 4
    has_above = above < n
    has_below = below >= 0

    rows, kv_width = k_hbm.shape
    ratio = q_hbm.shape[1] // kv_width
    chunks = kv_width // DH
    last = chunks - 1
    blocks = rows // BLK
    early = jnp.where(core == 0, 3, 1)
    late = 4 - early
    has_far = (far == 1) | has_below
    tops = slice(0, BLK)
    lows = slice(BLK, rows)
    whole = slice(0, rows)

    def routed(of_row):
        higher = last_row - of_row
        return jnp.where(
            higher > 0, jnp.minimum(chunks - ROUTED_SPARE, ROUTED_STEP * higher + ROUTED_BASE), 0
        )

    own_first = chunks - routed(row)
    below_first = chunks - routed(row - 1)

    def kv_cols(c, count=1):
        return pl.ds(pl.multiple_of(c * DH, DH), count * DH)

    def remote(src, dst, out, into, device):
        return pltpu.make_async_remote_copy(
            src_ref=src,
            dst_ref=dst,
            send_sem=send_sem.at[out],
            recv_sem=into,
            device_id={"seq": device},
            device_id_type=pl.DeviceIdType.MESH,
        )

    def send_own(slot, c, taken, out, into, device):
        for kind, hbm in enumerate((k_hbm, v_hbm)):
            remote(
                hbm.at[taken, kv_cols(c)],
                halo.at[kind, slot, taken, kv_cols(c)],
                out,
                into(kind),
                device,
            ).start()

    def send_held(src, dst, c, taken, out, into, device):
        remote(
            halo.at[:, src, taken, kv_cols(c)],
            halo.at[:, dst, taken, kv_cols(c)],
            out,
            into,
            device,
        ).start()

    def landed(ref, sem):
        pltpu.make_async_copy(ref, ref, sem).wait()

    def chunk_of(slot, c, taken=whole):
        return halo.at[:, slot, taken, kv_cols(c)]

    def by_half(half, act):
        @pl.when(half)
        def _():
            act(lows)

        @pl.when(jnp.logical_not(half))
        def _():
            act(whole)

    def upward(c):
        half = (place == 0) | ((place == 2) & (c >= own_first))
        by_half(half, lambda taken: send_own(0, c, taken, UP, lambda kind: z_recv.at[kind, c], above))

    def cross_start(c):
        for kind, hbm in enumerate((k_hbm, v_hbm)):
            remote(
                hbm.at[tops, kv_cols(c)],
                transit.at[kind, :, kv_cols(c)],
                CROSS,
                cross_recv.at[c // 2],
                across,
            ).start()

    def climb_start(c):
        remote(
            transit.at[:, :, kv_cols(c)],
            halo.at[:, 2, tops, kv_cols(c)],
            CLIMB,
            y_recv.at[c],
            above,
        ).start()

    barrier = pltpu.get_barrier_semaphore()

    def greet(device):
        pl.semaphore_signal(
            barrier, inc=1, device_id={"seq": device}, device_id_type=pl.DeviceIdType.MESH
        )

    greet(across)

    @pl.when(has_above)
    def _():
        greet(above)

    @pl.when(has_below)
    def _():
        greet(below)

    greet(partner)
    local = [
        pltpu.make_async_copy(k_hbm, own.at[0], local_sem.at[0]),
        pltpu.make_async_copy(v_hbm, own.at[1], local_sem.at[1]),
        pltpu.make_async_copy(q_hbm, q_own, local_sem.at[2]),
    ]
    docs = pltpu.make_async_copy(docs_hbm, docs_ref, local_sem.at[3])
    docs.start()
    for copy in local:
        copy.start()
    pl.semaphore_wait(barrier, 2 + has_above.astype(jnp.int32) + has_below.astype(jnp.int32))

    def first_sends(c, carry):
        @pl.when((place == 1) | ((place == 0) & (c < last)))
        def _():
            send_own(2, c, whole, OVER, lambda kind: y_recv.at[c], across)

        @pl.when(has_above & ((core == 1) | (c < UP_AHEAD)))
        def _():
            upward(c)

        @pl.when((place == 2) & (c < CROSS_AHEAD) & (own_first + c < chunks))
        def _():
            cross_start(own_first + c)

        @pl.when(core == 0)
        def _():
            given = last - c
            into = gift_recv.at[(given + 1) // chunks]
            send_own(1, given, whole, GIFT, lambda kind: into, partner)

        return carry

    lax.fori_loop(0, chunks, first_sends, 0)

    @pl.when(core == 1)
    def _():
        landed(chunk_of(1, last), gift_recv.at[1])

        @pl.when(far == 0)
        def _():
            send_held(1, 3, last, whole, EXTRA, pair_recv.at[last], across)

    @pl.when(jnp.logical_not(has_below))
    def _():
        for r in range(4):

            @pl.when((r == 0) | (r > place))
            def _():
                def clear(i, carry):
                    taken = pl.ds(pl.multiple_of(i * 16, 16), 16)
                    for kind in range(2):
                        halo[kind, r, taken, :] = jnp.zeros((16, kv_width), halo.dtype)
                    return carry

                lax.fori_loop(0, rows // 16, clear, 0)

    def shown(held, first):
        return jnp.concatenate(
            [
                jnp.full((1, BLK), jnp.where(b >= first, 0.0, HIDDEN), jnp.float32)
                for b in held
            ],
            axis=1,
        )

    docs.wait()
    second = jnp.where(place == 2, 1, 2)
    third = jnp.where(place == 2, 2, late)

    def slot_blocks(r):
        return [(me - r) * blocks + b for b in range(blocks)]

    hide_all = []
    hide_main = []
    hide_second = []
    hide_third = []
    for a in range(blocks):
        number = me * blocks + a
        end = jnp.int32(0)
        first = jnp.int32(0)
        for d in range(docs_ref.shape[0]):
            end = end + docs_ref[d]
            first = jnp.where(end <= number, end, first)
        oldest = slot_blocks(4)[a + 1 :]
        mine = slot_blocks(0)[: a + 1]
        between = slot_blocks(3) + slot_blocks(2) + slot_blocks(1)
        hide_all.append(shown(oldest + between + mine, first))
        hide_main.append(shown(oldest + slot_blocks(early) + mine, first))
        hide_second.append(shown(slot_blocks(second), first))
        hide_third.append(shown(slot_blocks(third), first))

    for copy in local:
        copy.wait()

    def heads_of(c):
        return [pl.ds(pl.multiple_of((c * ratio + g) * DH, DH), DH) for g in range(ratio)]

    def query_tile(c, a):
        return jnp.concatenate(
            [q_own[a * BLK : (a + 1) * BLK, hc] for hc in heads_of(c)], axis=0
        )

    def dot_keys(q_tile, keys):
        return lax.dot_general(
            q_tile, keys, (((1,), (1,)), ((), ())), preferred_element_type=jnp.float32
        )

    def gathered(kind, a, slots, cols):
        parts = []
        if a + 1 < blocks:
            parts.append(halo[kind, 0, (a + 1) * BLK :, cols])
        for r in slots:
            parts.append(halo[kind, r, :, cols])
        parts.append(own[kind, : (a + 1) * BLK, cols])
        return jnp.concatenate(parts, axis=0)

    def attend(c, slots, hide):
        q_index = lax.broadcasted_iota(jnp.int32, (BLK, BLK), 0)
        k_index = lax.broadcasted_iota(jnp.int32, (BLK, BLK), 1)
        causal = jnp.where(k_index <= q_index, 0.0, HIDDEN).astype(jnp.float32)
        causal = jnp.concatenate([causal] * ratio, axis=0)
        cols = kv_cols(c)
        kept = []
        for a in range(blocks):
            scores = dot_keys(query_tile(c, a), gathered(0, a, slots, cols)) + hide[a]
            scores = jnp.concatenate([scores[:, :-BLK], scores[:, -BLK:] + causal], axis=1)
            top = jnp.max(scores, axis=1, keepdims=True)
            weights = jnp.exp2((scores - top) * EXP2_SCALE)
            total = jnp.sum(weights, axis=1, keepdims=True)
            blended = jnp.dot(
                weights.astype(jnp.bfloat16),
                gathered(1, a, slots, cols),
                preferred_element_type=jnp.float32,
            )
            kept.append((top, total, blended))
        return kept

    def store(c, kept):
        for a in range(blocks):
            top, total, blended = kept[a]
            blended = (blended / total).astype(o_own.dtype)
            for g, hc in enumerate(heads_of(c)):
                o_own[a * BLK : (a + 1) * BLK, hc] = blended[g * BLK : (g + 1) * BLK]

    def merge(slot, hide, kept):
        merged = []
        cols = kv_cols(last)
        for a in range(blocks):
            top, total, blended = kept[a]
            scores = dot_keys(query_tile(last, a), halo[0, slot, :, cols]) + hide[a]
            new_top = jnp.maximum(top, jnp.max(scores, axis=1, keepdims=True))
            shrink = jnp.exp2((top - new_top) * EXP2_SCALE)
            weights = jnp.exp2((scores - new_top) * EXP2_SCALE)
            total = total * shrink + jnp.sum(weights, axis=1, keepdims=True)
            blended = blended * shrink + jnp.dot(
                weights.astype(jnp.bfloat16),
                halo[1, slot, :, cols],
                preferred_element_type=jnp.float32,
            )
            merged.append((new_top, total, blended))
        return merged

    def z_part(t):
        @pl.when(has_below)
        def _():
            half = (place == 0) | ((place == 2) & (t >= below_first))
            for kind in range(2):

                def pass_on(taken):
                    held = halo.at[kind, 0, taken, kv_cols(t)]
                    landed(held, z_recv.at[kind, t])

                    @pl.when(far == 1)
                    def _():
                        remote(
                            held,
                            halo.at[kind, 2, taken, kv_cols(t)],
                            OVER,
                            y_recv.at[t],
                            across,
                        ).start()

                by_half(half, pass_on)

            @pl.when((core == 1) & (t < last))
            def _():
                send_held(0, 3, t, whole, RISE, pair_recv.at[t], partner)

            @pl.when((core == 1) & (t == last))
            def _():
                send_held(0, 3, t, whole, RISE, rise_recv.at[0], partner)

        @pl.when(has_above)
        def _():
            ahead = own_first + t + CROSS_AHEAD

            @pl.when((place == 2) & (ahead < chunks))
            def _():
                cross_start(ahead)

            @pl.when((place == 0) & (own_first + t < chunks) & (lax.rem(t, 2) == 0))
            def _():
                c = own_first + t
                landed(transit.at[:, :, kv_cols(c, 2)], cross_recv.at[c // 2])
                climb_start(c)
                climb_start(c + 1)

            @pl.when((core == 0) & (t + UP_AHEAD < chunks))
            def _():
                upward(t + UP_AHEAD)

    def y_part(c):
        @pl.when(has_far)
        def _():
            landed(chunk_of(2, c), y_recv.at[c])
            send_held(2, 4 - late, c, whole, LATE, pair_recv.at[c], partner)

    def attend_all(c):
        both = (core == 0) & has_below

        @pl.when(both)
        def _():
            landed(halo.at[:, 0:2, :, kv_cols(c)], pair_recv.at[c])

        @pl.when(has_far & jnp.logical_not(both))
        def _():
            landed(chunk_of(late, c), pair_recv.at[c])

        store(c, attend(c, (3, 2, 1), hide_all))

    def z_lead(t, carry):
        z_part(t)
        return carry

    lax.fori_loop(0, Z_LEAD, z_lead, 0)

    def step_of(t, carry):
        @pl.when(t + Z_LEAD < chunks)
        def _():
            z_part(t + Z_LEAD)

        @pl.when(t >= 1)
        def _():
            y_part(t - 1)

        @pl.when((t == 2) & (core == 1))
        def _():
            landed(halo.at[:, 1, :, kv_cols(0, last)], gift_recv.at[0])

        @pl.when(t >= 2)
        def _():
            attend_all(t - 2)

        return carry

    lax.fori_loop(0, last, step_of, 0)

    @pl.when(Z_LEAD == 0)
    def _():
        z_part(last)

    attend_all(last - 2)

    @pl.when((core == 0) & has_below)
    def _():
        landed(chunk_of(3, last), rise_recv.at[0])

    kept = attend(last, (early,), hide_main)
    y_part(last - 1)
    attend_all(last - 1)

    @pl.when(has_far & (place != 2))
    def _():
        landed(chunk_of(2, last), y_recv.at[last])
        send_held(2, 4 - late, last, whole, LATE, pair_recv.at[last], partner)

    @pl.when(place == 2)
    def _():
        landed(chunk_of(1, last), pair_recv.at[last])

    kept = merge(second, hide_second, kept)

    @pl.when(has_far & (place != 2))
    def _():
        landed(chunk_of(late, last), pair_recv.at[last])

        @pl.when(place == 3)
        def _():
            send_held(3, 2, last, whole, EXTRA, y_recv.at[last], partner)

    @pl.when(place == 2)
    def _():
        landed(chunk_of(2, last), y_recv.at[last])

    store(last, merge(third, hide_third, kept))

    def drained(taken, width, out):
        landed(halo.at[:, 0, taken, 0:width], send_sem.at[out])

    @pl.when(has_above & (place == 0))
    def _():
        drained(lows, kv_width, UP)

    @pl.when(has_above & (core == 1))
    def _():
        drained(whole, kv_width, UP)

    @pl.when((place == 1) | ((place == 3) & has_below))
    def _():
        drained(whole, kv_width, OVER)

    @pl.when(place == 0)
    def _():
        drained(whole, last * DH, OVER)

    for r in range(last_row):
        count = min(chunks - ROUTED_SPARE, ROUTED_STEP * (last_row - r) + ROUTED_BASE)

        @pl.when((place == 2) & (row == r))
        def _():
            drained(whole, (2 * chunks - count) * DH // 2, UP)
            drained(tops, count * DH, CROSS)

        @pl.when((place == 2) & (row == r + 1))
        def _():
            drained(whole, (2 * chunks - count) * DH // 2, OVER)

        @pl.when((place == 0) & (row == r))
        def _():
            drained(tops, count * DH, CLIMB)

    @pl.when(core == 0)
    def _():
        drained(whole, kv_width, GIFT)

    @pl.when((core == 1) & has_below)
    def _():
        drained(whole, kv_width, RISE)

    @pl.when(has_far & (place != 2))
    def _():
        drained(whole, kv_width, LATE)

    @pl.when(place == 2)
    def _():
        drained(whole, last * DH, LATE)

    @pl.when(core == 1)
    def _():
        drained(whole, DH, EXTRA)


def on_paired_device(n, queries, keys, values, doc_blocks):
    rows, kv_width = keys.shape
    chunks = kv_width // DH
    return pl.pallas_call(
        functools.partial(paired_kernel, n),
        out_shape=pltpu.VMEM(queries.shape, queries.dtype),
        in_specs=[pl.BlockSpec(memory_space=pl.ANY)] * 4,
        out_specs=pl.BlockSpec(memory_space=pltpu.VMEM),
        scratch_shapes=[
            pltpu.VMEM(queries.shape, queries.dtype),
            pltpu.VMEM((2, rows, kv_width), keys.dtype),
            pltpu.VMEM((2, 4, rows, kv_width), keys.dtype),
            pltpu.VMEM((2, BLK, kv_width), keys.dtype),
            pltpu.SMEM(doc_blocks.shape, doc_blocks.dtype),
            pltpu.SemaphoreType.DMA((4,)),
            pltpu.SemaphoreType.DMA((2, chunks)),
            pltpu.SemaphoreType.DMA((chunks,)),
            pltpu.SemaphoreType.DMA((chunks,)),
            pltpu.SemaphoreType.DMA((chunks // 2,)),
            pltpu.SemaphoreType.DMA((2,)),
            pltpu.SemaphoreType.DMA((1,)),
            pltpu.SemaphoreType.DMA((8,)),
        ],
        compiler_params=pltpu.CompilerParams(
            collective_id=0, has_side_effects=True, vmem_limit_bytes=60 * 1024 * 1024
        ),
    )(doc_blocks, queries, keys, values)


def solution(mesh):
    n = mesh.shape["seq"]
    spread = P(("groups", "seq"), None)
    return jax.shard_map(
        functools.partial(on_paired_device if n // 4 == 4 else on_device, n),
        mesh=mesh,
        in_specs=(spread, spread, spread, P("groups")),
        out_specs=spread,
        check_vma=False,
    )
```
